32 devices in a mesh: prow: 4 (over x, core), pcol: 8 (over z, y).
Axes of the slice: x: 2, y: 2, z: 4, core: 2. Of those that a mesh axis runs over, the one named last changes fastest.
Arguments:
- panels: bfloat16 [2, 48, 2048, 256], P(None, 'pcol', 'prow'), may hold values from -0.59765625 to 0.59765625
- inverses: bfloat16 [2, 48, 256, 256], P(None, 'pcol', 'prow'), may hold values from -0.25 to 0.25
- dest: int32 [48, 8, 8], P('pcol', 'prow'), may hold values from 0 to 7, as said below
- target: int32 [48, 8, 8], P('pcol', 'prow'), may hold values from 0 to 1
- ancestors: float32 [2, 2048, 2048], P(None, 'prow', 'pcol'), may hold values from -6 to 6
Outputs:
- factor: bfloat16 [2, 48, 2048, 256], P(None, 'pcol', 'prow')
- schur: float32 [2, 2048, 2048], P(None, 'prow', 'pcol')
The draws below stay inside these ranges and needn't reach their ends.
Inputs may be any that keep to these rules, and one draw needn't show every extreme that they name: `dest`: among the 96 update blocks of one device (its leaves, its block rows), at most 24 name any one process column; on every process row one process column is named by exactly 24 blocks of every device of that row.
All inputs are finite; a program needn't handle non-finite values.
Results may differ from the reference program's by a relative error of at most 0.0045.
Values may be sent and summed in bfloat16 or wider, within the bound.
No kernel may reach another device: no remote copies, remote signals or barrier semaphores. Data moves between devices by JAX's collectives and lax.ppermute only.
A program may use at most 128 MiB of HBM per device.

```python
import jax
import jax.numpy as jnp
from jax import lax

W = 256
ROWB = 8
LEAF_DEV = 6
ANC_DEV = 2
CAP = 24
LEAVES = 48
FRONT = 2048
ANC_ROWS = 2048
ANC_COLS = 2048
N_PROW = 4
N_PCOL = 8


def draw_dest(key, part):
    rows_local = ROWB // N_PROW
    block_count = LEAF_DEV * rows_local * ROWB
    row_keys = jax.random.split(jax.random.fold_in(key, 11), N_PROW)

    def per_row(row_key):
        full_dest = jax.random.randint(jax.random.fold_in(row_key, 1), (), 0, N_PCOL).astype(jnp.int32)

        def per_device(device_key):
            others = (full_dest + 1 + jnp.arange((N_PCOL - 1) * CAP, dtype=jnp.int32) // CAP) % N_PCOL
            shuffled = jax.random.permutation(jax.random.fold_in(device_key, 2), others)
            chosen = jnp.concatenate([jnp.full((CAP,), full_dest, jnp.int32), shuffled[:block_count - CAP]])
            return jax.random.permutation(jax.random.fold_in(device_key, 3), chosen)
        return jax.vmap(per_device)(jax.random.split(jax.random.fold_in(row_key, 4), N_PCOL))
    layout = jax.vmap(per_row)(row_keys)
    layout = layout.reshape(N_PROW, N_PCOL, LEAF_DEV, rows_local, ROWB)
    return layout.transpose(1, 2, 0, 3, 4).reshape(LEAF_DEV * N_PCOL, ROWB, ROWB).astype(jnp.int32)


def touch_ends(result, stream_key, low, top_value):
    place = [jax.random.randint(jax.random.fold_in(stream_key, axis), (), 0, length) for axis, length in enumerate(result.shape)]
    longest = result.shape.index(max(result.shape))
    beside = place[:longest] + [(place[longest] + 1) % result.shape[longest]] + place[longest + 1:]
    return result.at[tuple(place)].set(low).at[tuple(beside)].set(top_value)


def block_scale(stream_key, dims, pieces, low, high):
    loudness = 1.0
    for position, blocks in pieces:
        heights = jax.random.uniform(jax.random.fold_in(jax.random.fold_in(stream_key, 6), position), (blocks,), jnp.float32, low / len(pieces), high / len(pieces))
        loudness = loudness * jnp.repeat(jnp.exp(heights), dims[position] // blocks).reshape((-1,) + (1,) * (len(dims) - 1 - position))
    return loudness


def bell_draw(rng, shape, spread, bound, shards=(), kind=jnp.bfloat16):
    values = spread * jax.random.normal(rng, shape, jnp.float32)
    if shards:
        values = values * block_scale(rng, shape, shards, -0.22, 0.18)
    return jnp.clip(values, -bound, bound).astype(kind)


def setup_inputs(seed: int = 0) -> dict:
    keys = jax.random.split(jax.random.key(seed), 6)
    return {
        "panels": bell_draw(keys[0], (2, LEAVES, FRONT, W), 0.1, 0.59765625, ((1, 8), (2, 4))),
        "inverses": bell_draw(keys[1], (2, LEAVES, W, W), (2 * W) ** -0.5, 0.25, ((1, 8), (2, 4))),
        "dest": draw_dest(jax.random.fold_in(keys[5], 71), 0),
        "target": touch_ends(jax.random.randint(keys[3], (LEAVES, ROWB, ROWB), 0, ANC_DEV), jax.random.fold_in(keys[3], 1), 0, ANC_DEV - 1).astype(jnp.int32),
        "ancestors": bell_draw(keys[4], (2, ANC_ROWS, ANC_COLS), 1.0, 6.0, ((1, 4), (2, 8)), jnp.float32),
    }


def complex_dot(left_side, right_side):
    real_part = jnp.dot(left_side[0], right_side[0], preferred_element_type=jnp.float32) - jnp.dot(left_side[1], right_side[1], preferred_element_type=jnp.float32)
    imag_part = jnp.dot(left_side[0], right_side[1], preferred_element_type=jnp.float32) + jnp.dot(left_side[1], right_side[0], preferred_element_type=jnp.float32)
    return jnp.stack([real_part, imag_part])


def reference(panels, inverses, dest, target, ancestors):
    rows_local = ROWB // N_PROW
    block_rows = jnp.arange(ROWB, dtype=jnp.int32)[:, None] // rows_local

    def per_leaf(totals, inputs):
        panel, inverse, leaf_dest, leaf_target = inputs
        lower_panel = complex_dot(panel, inverse).astype(jnp.bfloat16)
        update = complex_dot(lower_panel, jnp.swapaxes(panel, 1, 2)).astype(jnp.bfloat16)
        update = lax.optimization_barrier(update).astype(jnp.float32)
        blocks = update.reshape(2, ROWB, W, ROWB, W).transpose(1, 3, 0, 2, 4).reshape(ROWB * ROWB, 2, W, W)
        index = ((block_rows * ANC_DEV + leaf_target) * N_PCOL + leaf_dest).reshape(-1).astype(jnp.int32)
        return totals.at[index].add(blocks), lower_panel

    initial = jnp.zeros((N_PROW * ANC_DEV * N_PCOL, 2, W, W), jnp.float32)
    totals, lowers = lax.scan(per_leaf, initial, (panels.transpose(1, 0, 2, 3), inverses.transpose(1, 0, 2, 3), dest, target))
    factor = lowers.transpose(1, 0, 2, 3)
    layout = totals.reshape(N_PROW, ANC_DEV, N_PCOL, 2, W, W).transpose(3, 0, 1, 4, 2, 5)
    layout = layout.reshape(2, N_PROW * ANC_DEV * W, N_PCOL * W)
    return factor, ancestors - layout
```

```python
import functools

import jax
import jax.numpy as jnp
from jax import lax
from jax.experimental import pallas as pl
from jax.experimental.pallas import tpu as pltpu
from jax.sharding import PartitionSpec as P

CHUNKS = (2, 2, 2, 1, 1)


def swap(value, axis, bit):
    size = lax.axis_size(axis)
    return lax.ppermute(value, axis, [(i, i ^ bit) for i in range(size)])


def gather_xor(own, axis):
    pieces = {0: own}
    bit = lax.axis_size(axis) // 2
    while bit:
        pieces.update({j ^ bit: swap(piece, axis, bit) for j, piece in list(pieces.items())})
        bit //= 2
    return [pieces[j] for j in range(len(pieces))]


def dot_nn(left, right):
    return lax.dot_general(left, right, (((1,), (0,)), ((), ())), preferred_element_type=jnp.float32)


def dot_nt(left, right):
    return lax.dot_general(left, right, (((1,), (1,)), ((), ())), preferred_element_type=jnp.float32)


def factor_body(ids, panel, *refs):
    pieces, out, inverse = refs[:-2], refs[-2], refs[-1]
    rows = pieces[0].shape[2]
    for j, piece in enumerate(pieces):
        start = pl.multiple_of((ids[0] ^ j) * rows, rows)
        inverse[:, pl.ds(start, rows), :] = piece[:, 0]
    panel_real, panel_imag = panel[0, 0], panel[1, 0]
    real, imag = inverse[0], inverse[1]
    out[0, 0] = (dot_nn(panel_real, real) - dot_nn(panel_imag, imag)).astype(out.dtype)
    out[1, 0] = (dot_nn(panel_real, imag) + dot_nn(panel_imag, real)).astype(out.dtype)


def factor_kernel(ids, panels, pieces):
    _, leaves, rows, width = panels.shape
    piece_rows = pieces[0].shape[2]
    panel_spec = pl.BlockSpec((2, 1, rows, width), lambda s: (0, s, 0, 0))
    piece_spec = pl.BlockSpec((2, 1, piece_rows, width), lambda s: (0, s, 0, 0))
    return pl.pallas_call(
        factor_body,
        grid=(leaves,),
        in_specs=[pl.BlockSpec(memory_space=pltpu.SMEM), panel_spec] + [piece_spec] * len(pieces),
        out_specs=panel_spec,
        out_shape=jax.ShapeDtypeStruct(panels.shape, panels.dtype),
        scratch_shapes=[pltpu.VMEM((2, width, width), panels.dtype)],
        cost_estimate=pl.CostEstimate(
            flops=8 * leaves * rows * width * width, bytes_accessed=4 * panels.size, transcendentals=0
        ),
        name="factor",
    )(ids, panels, *pieces)


def update_body(ids, dest, target, factor, *refs, owned):
    count = len(refs) - 7
    pieces = refs[:count]
    keep, send, factor_buf, piece_buf, total, factor_sem, piece_sem = refs[count:]
    _, leaves, rows, width = factor.shape
    local_rows = rows // width
    cols = pieces[0].shape[3]

    def copies(s):
        yield pltpu.make_async_copy(factor.at[:, s], factor_buf.at[s], factor_sem.at[s])
        for j, piece in enumerate(pieces):
            yield pltpu.make_async_copy(piece.at[:, s], piece_buf.at[s, :, j], piece_sem.at[s, j])

    for s in range(leaves):
        for copy in copies(s):
            copy.start()
    total[...] = jnp.zeros(total.shape, total.dtype)

    def leaf(s, carry):
        for copy in copies(s):
            copy.wait()
        panel_real = piece_buf[s, 0].reshape(count * local_rows * cols, width)
        panel_imag = piece_buf[s, 1].reshape(count * local_rows * cols, width)
        for a in range(local_rows):
            real = factor_buf[s, 0, a * width : (a + 1) * width, :]
            imag = factor_buf[s, 1, a * width : (a + 1) * width, :]
            update_real = dot_nt(panel_real, real) + dot_nt(panel_imag, -imag)
            update_imag = dot_nt(panel_real, imag) + dot_nt(panel_imag, real)
            for block in range(count * local_rows):
                j, i = divmod(block, local_rows)
                b = (ids[0] ^ j) * local_rows + i
                slot = (dest[s, a, b] ^ ids[1]) * owned + target[s, a, b]
                total[slot, 0] += update_real[block * cols : (block + 1) * cols]
                total[slot, 1] += update_imag[block * cols : (block + 1) * cols]
        return carry

    lax.fori_loop(0, leaves, leaf, 0)
    for d in range(keep.shape[0]):
        for t in range(owned):
            keep[d, t] = total[2 * d * owned + t]
            send[d, t] = total[(2 * d + 1) * owned + t].astype(send.dtype)


def update_kernel(ids, dest, target, factor, pieces, owned, columns):
    _, leaves, rows, width = factor.shape
    local_rows = rows // width
    cols = pieces[0].shape[3]
    half = (columns // 2, owned, 2, cols, width)
    smem = pl.BlockSpec(memory_space=pltpu.SMEM)
    hbm = pl.BlockSpec(memory_space=pl.ANY)
    vmem = pl.BlockSpec(memory_space=pltpu.VMEM)
    return pl.pallas_call(
        functools.partial(update_body, owned=owned),
        in_specs=[smem] * 3 + [hbm] * (1 + len(pieces)),
        out_specs=[vmem, vmem],
        out_shape=[jax.ShapeDtypeStruct(half, jnp.float32), jax.ShapeDtypeStruct(half, jnp.bfloat16)],
        scratch_shapes=[
            pltpu.VMEM((leaves, 2, rows, width), factor.dtype),
            pltpu.VMEM((leaves, 2, len(pieces), local_rows, cols, width), factor.dtype),
            pltpu.VMEM((columns * owned, 2, cols, width), jnp.float32),
            pltpu.SemaphoreType.DMA((leaves,)),
            pltpu.SemaphoreType.DMA((leaves, len(pieces))),
        ],
        cost_estimate=pl.CostEstimate(
            flops=8 * leaves * rows * len(pieces) * local_rows * cols * width,
            bytes_accessed=2 * factor.size + 2 * len(pieces) * pieces[0].size,
            transcendentals=0,
        ),
        name="update",
    )(ids, dest, target, factor, *pieces)


def final_body(ancestors, *refs):
    out = refs[-1]
    owned = refs[0].shape[0]
    width = out.shape[2]
    for t in range(owned):
        for plane in range(2):
            total = jnp.concatenate(
                [keep[t, plane] + got[t, plane].astype(jnp.float32) for keep, got in zip(refs[:-1:2], refs[1:-1:2])],
                axis=0,
            )
            rows = slice(t * width, (t + 1) * width)
            out[plane, rows, :] = ancestors[plane, rows, :] - total.T


def final_kernel(ancestors, sums):
    vmem = pl.BlockSpec(memory_space=pltpu.VMEM)
    flat = [part for pair in sums for part in pair]
    return pl.pallas_call(
        final_body,
        in_specs=[vmem] * (1 + len(flat)),
        out_specs=vmem,
        out_shape=jax.ShapeDtypeStruct(ancestors.shape, ancestors.dtype),
        name="final",
    )(ancestors, *flat)


def local(panels, inverses, dest, target, ancestors):
    _, leaves, rows, width = panels.shape
    local_rows = rows // width
    owned = ancestors.shape[1] // width
    columns = lax.axis_size("pcol")
    ids = jnp.stack([lax.axis_index("prow"), lax.axis_index("pcol")]).astype(jnp.int32)
    factor = factor_kernel(ids, panels, gather_xor(inverses, "prow"))
    grouped = panels.reshape(2, leaves, local_rows, width, width)
    sums = []
    start = 0
    for part in CHUNKS:
        cols = part * width // sum(CHUNKS)
        pieces = gather_xor(grouped[:, :, :, start : start + cols, :], "prow")
        start += cols
        keep, send = update_kernel(ids, dest, target, factor, pieces, owned, columns)
        bit = 1
        while True:
            got = swap(send, "pcol", bit)
            bit *= 2
            if bit == columns:
                break
            both = keep + got.astype(keep.dtype)
            both = both.reshape((both.shape[0] // 2, 2) + both.shape[1:])
            keep, send = both[:, 0], both[:, 1].astype(jnp.bfloat16)
        sums.append((keep[0], got[0]))
    return factor, final_kernel(ancestors, sums)


def solution(mesh):
    return jax.shard_map(
        local,
        mesh=mesh,
        in_specs=(
            P(None, "pcol", "prow", None),
            P(None, "pcol", "prow", None),
            P("pcol", "prow", None),
            P("pcol", "prow", None),
            P(None, "prow", "pcol"),
        ),
        out_specs=(P(None, "pcol", "prow", None), P(None, "prow", "pcol")),
        check_vma=False,
    )
```
